512 devices in a mesh: rows: 32 (over z, x), tp: 2 (over core), job: 8 (over y).
Axes of the slice: x: 4, y: 8, z: 8, core: 2. Of those that a mesh axis runs over, the one named last changes fastest.
Arguments:
- train_query: bfloat16 [16384, 2048], P(('job', 'rows'), 'tp'), parts along dimension 0, may hold values from -0.125 to 0.125
- low_query: bfloat16 [16384, 16], P(('job', 'rows')), parts along dimension 0, may hold values from -0.125 to 0.125
- high_query: bfloat16 [128, 2048], P('job', 'tp'), parts along dimension 0, may hold values from -1.5 to 1.5
- train_key: bfloat16 [16384, 512], P(('job', 'rows'), 'tp'), parts along dimension 0, may hold values from -0.125 to 0.125
- low_key: bfloat16 [16384, 16], P(('job', 'rows')), parts along dimension 0, may hold values from -0.125 to 0.125
- high_key: bfloat16 [128, 512], P('job', 'tp'), parts along dimension 0, may hold values from -1.5 to 1.5
- train_value: bfloat16 [16384, 512], P(('job', 'rows'), 'tp'), parts along dimension 0, may hold values from -0.125 to 0.125
- low_value: bfloat16 [16384, 16], P(('job', 'rows')), parts along dimension 0, may hold values from -0.125 to 0.125
- high_value: bfloat16 [128, 512], P('job', 'tp'), parts along dimension 0, may hold values from -1.5 to 1.5
- norm_train: float32 [16384], P(('job', 'rows', 'tp')), parts along dimension 0, may hold values from 0.25 to 1.75
- norm_step: float32 [16384], P(('job', 'rows', 'tp')), parts along dimension 0, may hold values from -0.3 to 0.3
Outputs:
- serve_query: bfloat16 [16384, 2048], P(('job', 'tp')), parts along dimension 0
- serve_key: bfloat16 [4096, 2048], P(('job', 'tp')), parts along dimension 0
- serve_value: bfloat16 [4096, 2048], P(('job', 'tp')), parts along dimension 0
- serve_norm: bfloat16 [16384], P('job'), parts along dimension 0
The draws below stay inside these ranges and needn't reach their ends.
There are 8 independent parts, one for each index of `job`. The reference program is written for one: setup_inputs(seed, part) draws one part's arguments, and reference() takes and returns one part's arrays. A program takes and returns all parts, laid end to end along the dimension named above; each array names one. Nothing has to cross between parts.
All inputs are finite; a program needn't handle non-finite values.
Results may differ from the reference program's by a relative error of at most 0.001.
Values may be sent and summed in bfloat16 or wider, within the bound.
No kernel may reach another device: no remote copies, remote signals or barrier semaphores. Data moves between devices by JAX's collectives and lax.ppermute only.
A program may use at most 64 MiB of HBM per device.

```python
import jax
import jax.numpy as jnp

D_MODEL = 2048
Q_DIM = 2048
KV_DIM = 512
RANK = 16


def level_of(stream_key, extent, pieces, low, top_value):
    gain = 1.0
    for dim, blocks in pieces:
        heights = jax.random.uniform(jax.random.fold_in(jax.random.fold_in(stream_key, 6), dim), (blocks,), jnp.float32, low / len(pieces), top_value / len(pieces))
        gain = gain * jnp.repeat(jnp.exp(heights), extent[dim] // blocks).reshape((-1,) + (1,) * (len(extent) - 1 - dim))
    return gain


def centred(own_key, shape, spread, reach, cuts=(), kind=jnp.bfloat16):
    entries = spread * jax.random.normal(own_key, shape, jnp.float32)
    if cuts:
        entries = entries * level_of(own_key, shape, cuts, -0.22, 0.18)
    return jnp.clip(entries, -reach, reach).astype(kind)


def setup_inputs(seed: int = 0, part: int = 0) -> dict:
    key_of = jax.random.split(jax.random.key(seed), 12)
    own_keys = jax.random.split(jax.random.fold_in(key_of[11], part), 12)
    return {
        "train_query": centred(own_keys[0], (D_MODEL, Q_DIM), D_MODEL ** -0.5, 0.125, ((0, 32), (1, 2))),
        "low_query": centred(own_keys[1], (D_MODEL, RANK), D_MODEL ** -0.5, 0.125, ((0, 32),)),
        "high_query": centred(own_keys[2], (RANK, Q_DIM), RANK ** -0.5, 1.5, ((1, 2),)),
        "train_key": centred(own_keys[3], (D_MODEL, KV_DIM), D_MODEL ** -0.5, 0.125, ((0, 32), (1, 2))),
        "low_key": centred(own_keys[4], (D_MODEL, RANK), D_MODEL ** -0.5, 0.125, ((0, 32),)),
        "high_key": centred(own_keys[5], (RANK, KV_DIM), RANK ** -0.5, 1.5, ((1, 2),)),
        "train_value": centred(own_keys[6], (D_MODEL, KV_DIM), D_MODEL ** -0.5, 0.125, ((0, 32), (1, 2))),
        "low_value": centred(own_keys[7], (D_MODEL, RANK), D_MODEL ** -0.5, 0.125, ((0, 32),)),
        "high_value": centred(own_keys[8], (RANK, KV_DIM), RANK ** -0.5, 1.5, ((1, 2),)),
        "norm_train": jnp.clip(1.0 + 0.15 * jax.random.normal(own_keys[9], (D_MODEL,), jnp.float32), 0.25, 1.75),
        "norm_step": jnp.clip(jax.random.uniform(own_keys[10], (D_MODEL,), jnp.float32, -0.3, 0.3) * level_of(own_keys[10], (D_MODEL,), ((0, 64),), -0.4, 0.0), -0.3, 0.3),
    }


mix_rate = 0.5


def reference(train_query, low_query, high_query, train_key, low_key, high_key, train_value, low_value, high_value, norm_train, norm_step):
    fresh_query = train_query.astype(jnp.float32) + mix_rate * jnp.dot(low_query, high_query, preferred_element_type=jnp.float32)
    fresh_key = train_key.astype(jnp.float32) + mix_rate * jnp.dot(low_key, high_key, preferred_element_type=jnp.float32)
    fresh_value = train_value.astype(jnp.float32) + mix_rate * jnp.dot(low_value, high_value, preferred_element_type=jnp.float32)
    serve_query = fresh_query.T.astype(jnp.bfloat16)
    serve_key = fresh_key.T.astype(jnp.bfloat16)
    serve_value = fresh_value.T.astype(jnp.bfloat16)
    serve_norm = (norm_train + norm_step).astype(jnp.bfloat16)
    return serve_query, serve_key, serve_value, serve_norm
```

```python
import functools

import jax
import jax.numpy as jnp
from jax import lax
from jax.experimental import pallas as pl
from jax.experimental.pallas import tpu as pltpu
from jax.sharding import Mesh, PartitionSpec as P


mix_rate = 0.5
LANES = 128
NORM_ROWS = 8
A_Q = 2
B_CUTS = (6,)


def merge_kernel(
    tq, lq, hq, tk, lk, hk, tv, lv, hv, nt, ns, *outs
):
    out_a, outs_b = outs[0], outs[1:]

    def piece(t, l, h, lo, hi):
        low_high = lax.dot_general(
            l[...], h[:, lo:hi], (((0,), (0,)), ((), ())), preferred_element_type=jnp.float32
        )
        return (t[:, lo:hi].astype(jnp.float32) + mix_rate * low_high).astype(jnp.bfloat16)

    rows = tq.shape[0]
    at = A_Q * LANES
    for k, cut in enumerate(B_CUTS):
        w = piece(tq, lq, hq, at, at + cut * LANES)
        at += cut * LANES
        for d in range(outs_b[k].shape[0]):
            for j in range(cut):
                outs_b[k][d, j * rows : (j + 1) * rows, :] = w[:, j * LANES : (j + 1) * LANES]
    norm = (nt[...] + ns[...]).astype(jnp.bfloat16)
    norm = jnp.concatenate([norm, jnp.zeros((1, LANES - norm.shape[1]), jnp.bfloat16)], axis=1)
    norm = jnp.broadcast_to(norm, (NORM_ROWS, LANES))
    for d in range(outs_b[0].shape[0]):
        outs_b[0][d, B_CUTS[0] * rows :, :] = norm
    at = 0
    for t, l, h, width in ((tk, lk, hk, tk.shape[1]), (tv, lv, hv, tv.shape[1]), (tq, lq, hq, A_Q * LANES)):
        w = piece(t, l, h, 0, width)
        out_a[:, at : at + width] = w
        at += width


def turn_kernel(steps, *refs):
    pieces, (out, held) = refs[: len(steps)], refs[len(steps) :]
    n = len(steps)
    rows, width = pieces[0].shape
    me = lax.axis_index("x")
    for step, piece in zip(steps, pieces):
        at = pl.multiple_of(lax.rem(me + (step + n), n) * rows, rows)
        held[pl.ds(at, rows), :] = piece[...]
    for j in range(width // LANES):
        out[j * LANES : (j + 1) * LANES, :] = held[:, j * LANES : (j + 1) * LANES].T


def place_b_kernel(first, cut, rows, b, *rest):
    out, held, sem = rest[-3:]
    nx, nz = b.shape[0], b.shape[1]
    wide = nx * rows
    copies = []
    for j in range(cut):
        for z in range(nz):
            block = jnp.concatenate(
                [b[x, z, j * rows : (j + 1) * rows, :] for x in range(nx)], axis=0
            )
            held[j * LANES : (j + 1) * LANES, z * wide : (z + 1) * wide] = block.T
        copy = pltpu.make_async_copy(
            held.at[pl.ds(j * LANES, LANES), :],
            out.at[pl.ds((first + j) * LANES, LANES), :],
            sem.at[j],
        )
        copy.start()
        copies.append(copy)
    for copy in copies:
        copy.wait()


def place_a_kernel(steps, nz, wide, kv, *refs):
    n = len(steps)
    blocks = refs[:n]
    out_q, out_k, out_v, sem = refs[-4:]
    me = lax.axis_index("z")
    copies = []
    for i, (step, block) in enumerate(zip(steps, blocks)):
        at = pl.ds(pl.multiple_of(lax.rem(me + (step + nz), nz) * wide, wide), wide)
        for s, (lo, hi, out) in enumerate(
            ((0, kv, out_k), (kv, 2 * kv, out_v), (2 * kv, 2 * kv + A_Q * LANES, out_q))
        ):
            copy = pltpu.make_async_copy(
                block.at[pl.ds(lo, hi - lo), :], out.at[pl.ds(0, hi - lo), at], sem.at[i, s]
            )
            copy.start()
            copies.append(copy)
    for copy in copies:
        copy.wait()


def fan_kernel(b, out):
    for d in range(out.shape[0]):
        out[d] = b[...]


VM = pl.BlockSpec(memory_space=pltpu.VMEM)
ANY = pl.BlockSpec(memory_space=pl.ANY)


def call(kernel, ins, out_specs, out_shape, scratch=(), aliases={}, n_any=0, cost=1 << 20):
    return pl.pallas_call(
        kernel,
        in_specs=[VM] * (len(ins) - n_any) + [ANY] * n_any,
        out_specs=out_specs,
        out_shape=out_shape,
        scratch_shapes=list(scratch),
        input_output_aliases=aliases,
        cost_estimate=pl.CostEstimate(flops=cost, bytes_accessed=cost, transcendentals=0),
    )(*ins)


def shift(a, axis, by):
    n = lax.axis_size(axis)
    return lax.ppermute(a, axis, [(i, (i + by) % n) for i in range(n)])


def spread(a, axis):
    return lax.all_to_all(a, axis, 0, 0, tiled=True)


def steps_of(tq, lq, hq, tk, lk, hk, tv, lv, hv, nt, ns):
    nz, nx = lax.axis_size("z"), lax.axis_size("x")
    rows, q_wide = tq.shape
    kv = tk.shape[1]
    wide = nx * rows
    a_wide = 2 * kv + A_Q * LANES
    bf = jnp.bfloat16
    b_rows = [cut * rows + (NORM_ROWS if k == 0 else 0) for k, cut in enumerate(B_CUTS)]
    out_shape = [jax.ShapeDtypeStruct((rows, a_wide), bf)] + [
        jax.ShapeDtypeStruct((nz, r, LANES), bf) for r in b_rows
    ]
    a, *bs = call(
        merge_kernel,
        (tq, lq.T, hq, tk, lk.T, hk, tv, lv.T, hv, nt[None], ns[None]),
        [VM] * len(out_shape),
        out_shape,
    )
    b1 = []
    for b in bs:
        b1.append(spread(b, "z"))
    a1 = shift(a, "x", 1)
    a2 = shift(a, "x", -1)
    a3 = shift(a, "x", 2)
    own = call(
        functools.partial(turn_kernel, (0, -1, 1, -2)),
        (a, a1, a2, a3),
        VM,
        jax.ShapeDtypeStruct((a_wide, wide), bf),
        scratch=[pltpu.VMEM((wide, a_wide), bf)],
    )
    blocks = {0: own}
    for step in range(1, nz // 2):
        blocks[-step] = shift(blocks[1 - step], "z", 1)
        blocks[step] = shift(blocks[step - 1], "z", -1)
    blocks[-(nz // 2)] = shift(blocks[1 - nz // 2], "z", 1)
    b2 = []
    for b in b1:
        wide_b = call(fan_kernel, (b,), VM, jax.ShapeDtypeStruct((nx, *b.shape), bf))
        b2.append(spread(wide_b, "x"))
    q_shape = jax.ShapeDtypeStruct((q_wide, nz * wide), bf)
    kv_shape = jax.ShapeDtypeStruct((kv, nz * wide), bf)

    def place_b(k, out_q):
        first = A_Q + sum(B_CUTS[:k])
        cut = B_CUTS[k]
        ins = (b2[k],) if out_q is None else (b2[k], out_q)
        return call(
            functools.partial(place_b_kernel, first, cut, rows),
            ins,
            ANY,
            q_shape,
            scratch=[pltpu.VMEM((cut * LANES, nz * wide), bf), pltpu.SemaphoreType.DMA((cut,))],
            aliases={} if out_q is None else {1: 0},
            n_any=len(ins) - 1,
        )

    def place_a(steps, outs):
        ins = tuple(blocks[s] for s in steps) + outs
        n = len(steps)
        return call(
            functools.partial(place_a_kernel, steps, nz, wide, kv),
            ins,
            [ANY] * 3,
            [q_shape, kv_shape, kv_shape],
            scratch=[pltpu.SemaphoreType.DMA((n, 3))],
            aliases={n + i: i for i in range(len(outs))},
            n_any=len(outs),
        )

    half = nz // 2
    early = (0, -1, 1, -2, 2)
    late = tuple(s for s in (-3, 3, -half))
    outs = place_a(early, ())
    out_q = outs[0]
    for k in range(len(B_CUTS)):
        out_q = place_b(k, out_q)
    serve_query, serve_key, serve_value = place_a(late, (out_q, outs[1], outs[2]))
    part = nt.shape[0]
    mine = b2[0][:, :, B_CUTS[0] * rows, :part]
    mine = jnp.swapaxes(mine, 0, 1).reshape(nz * nx, part)
    other = lax.ppermute(mine, "tp", [(0, 1), (1, 0)])
    first = lax.axis_index("tp") == 0
    serve_norm = jnp.concatenate(
        [jnp.where(first, mine, other), jnp.where(first, other, mine)], axis=1
    ).reshape(-1)
    return serve_query, serve_key, serve_value, serve_norm


def solution(mesh):
    rows, tp, job = mesh.devices.shape
    nx = 4
    fine = Mesh(mesh.devices.reshape(rows // nx, nx, tp, job), ("z", "x", "tp", "job"))
    r = ("job", "z", "x")
    w, low, high, vec = P(r, "tp"), P(r, None), P("job", "tp"), P(("job", "z", "x", "tp"))
    out_specs = (P(("job", "tp"), None),) * 3 + (P("job"),)
    return jax.shard_map(
        steps_of,
        mesh=fine,
        in_specs=(w, low, high) * 3 + (vec, vec),
        out_specs=out_specs,
        check_vma=False,
    )
```

```python
import functools

import jax
import jax.numpy as jnp
from jax import lax
from jax.experimental import pallas as pl
from jax.experimental.pallas import tpu as pltpu
from jax.sharding import Mesh, PartitionSpec as P


mix_rate = 0.5
LANES = 128
NORM_ROWS = 8
A_Q = 2
B_CUTS = (6,)


def merged(t, l, h, lo, hi):
    low_high = lax.dot_general(
        l[...], h[:, lo:hi], (((0,), (0,)), ((), ())), preferred_element_type=jnp.float32
    )
    return (t[:, lo:hi].astype(jnp.float32) + mix_rate * low_high).astype(jnp.bfloat16)


def merge_kernel(tq, lq, hq, tk, lk, hk, tv, lv, hv, nt, ns, out_b, out_a):
    rows = tq.shape[0]
    w = merged(tq, lq, hq, A_Q * LANES, tq.shape[1])
    for d in range(out_b.shape[0]):
        for j in range(w.shape[1] // LANES):
            out_b[d, j * rows : (j + 1) * rows, :] = w[:, j * LANES : (j + 1) * LANES]
    at = 0
    for t, l, h, width in (
        (tk, lk, hk, tk.shape[1]),
        (tv, lv, hv, tv.shape[1]),
        (tq, lq, hq, A_Q * LANES),
    ):
        out_a[:rows, at : at + width] = merged(t, l, h, 0, width)
        at += width
    norm = nt[...] + ns[...]
    norm = jnp.concatenate([norm, jnp.zeros((1, LANES - norm.shape[1]), jnp.float32)], axis=1)
    norm = jnp.broadcast_to(norm, (NORM_ROWS, LANES)).astype(jnp.bfloat16)
    out_a[rows:, :LANES] = norm
    out_a[rows:, LANES:] = jnp.zeros((NORM_ROWS, out_a.shape[1] - LANES), jnp.bfloat16)


def turn_kernel(rows, part, a, out, out_norm):
    n, _, width = a.shape
    for j in range(width // LANES):
        block = jnp.concatenate(
            [a[x, :rows, j * LANES : (j + 1) * LANES] for x in range(n)], axis=0
        )
        out[j * LANES : (j + 1) * LANES, :] = block.T
    norm = jnp.concatenate([a[x, rows:, :part] for x in range(n)], axis=1)
    out_norm[...] = norm
    out[width:, : n * part] = norm
    out[width:, n * part :] = jnp.zeros((NORM_ROWS, out.shape[1] - n * part), jnp.bfloat16)


def place_b_kernel(first, cut, rows, b, *rest):
    out, held, sem = rest[-3:]
    nx, nz = b.shape[0], b.shape[1]
    wide = nx * rows
    copies = []
    for j in range(cut):
        for z in range(nz):
            block = jnp.concatenate(
                [b[x, z, j * rows : (j + 1) * rows, :] for x in range(nx)], axis=0
            )
            held[j * LANES : (j + 1) * LANES, z * wide : (z + 1) * wide] = block.T
        copy = pltpu.make_async_copy(
            held.at[pl.ds(j * LANES, LANES), :],
            out.at[pl.ds((first + j) * LANES, LANES), :],
            sem.at[j],
        )
        copy.start()
        copies.append(copy)
    for copy in copies:
        copy.wait()


def place_a(steps, nz, wide, kv, blocks, out_q, out_k, out_v, sem):
    me = lax.axis_index("z")
    end = 2 * kv + A_Q * LANES
    copies = []
    for i, (step, block) in enumerate(zip(steps, blocks)):
        z = lax.rem(me + (step + nz), nz)
        at = pl.ds(pl.multiple_of(z * wide, wide), wide)
        for s, (lo, hi, out) in enumerate(
            ((0, kv, out_k), (kv, 2 * kv, out_v), (2 * kv, end, out_q))
        ):
            copy = pltpu.make_async_copy(
                block.at[pl.ds(lo, hi - lo), :], out.at[pl.ds(0, hi - lo), at], sem.at[i, s]
            )
            copy.start()
            copies.append(copy)
    return copies


def early_kernel(steps, nz, wide, kv, *refs):
    n = len(steps)
    blocks, far = refs[:n], refs[n]
    out_q, out_k, out_v, out_n, held, sem = refs[n + 1 :]
    copies = place_a(steps, nz, wide, kv, blocks, out_q, out_k, out_v, sem)
    me = lax.axis_index("z")
    end = 2 * kv + A_Q * LANES
    lanes = held.shape[1]
    rows = [block[end:, :lanes] for block in blocks] + [far[...]]
    for step, row in zip(steps + (nz // 2,), rows):
        held[pl.ds(lax.rem(me + (step + nz), nz), 1), :] = row.astype(jnp.float32)[:1, :]
    out_n[...] = held[...].astype(out_n.dtype)
    for copy in copies:
        copy.wait()


def late_kernel(steps, nz, wide, kv, *refs):
    n = len(steps)
    copies = place_a(steps, nz, wide, kv, refs[:n], *refs[-4:])
    for copy in copies:
        copy.wait()


def norm_kernel(part, mine, other, out):
    m, o = mine[...].astype(jnp.float32), other[...].astype(jnp.float32)
    first = lax.axis_index("tp") == 0
    halves = (jnp.where(first, m, o), jnp.where(first, o, m))
    pieces = []
    for x in range(m.shape[1] // part):
        pieces += [half[:, x * part : (x + 1) * part] for half in halves]
    out[...] = jnp.concatenate(pieces, axis=1).astype(out.dtype)


def fan_kernel(b, out, sem):
    copies = [pltpu.make_async_copy(b, out.at[d], sem.at[d]) for d in range(out.shape[0])]
    for copy in copies:
        copy.start()
    for copy in copies:
        copy.wait()


VM = pl.BlockSpec(memory_space=pltpu.VMEM)
ANY = pl.BlockSpec(memory_space=pl.ANY)
HBM = pl.BlockSpec(memory_space=pltpu.HBM)


def call(kernel, ins, out_specs, out_shape, scratch=(), aliases={}, n_any=0, cost=1 << 20, vmem=16 << 20):
    return pl.pallas_call(
        kernel,
        in_specs=[VM] * (len(ins) - n_any) + [ANY] * n_any,
        out_specs=out_specs,
        out_shape=out_shape,
        scratch_shapes=list(scratch),
        input_output_aliases=aliases,
        compiler_params=pltpu.CompilerParams(vmem_limit_bytes=vmem),
        cost_estimate=pl.CostEstimate(flops=cost, bytes_accessed=cost, transcendentals=0),
    )(*ins)


def shift(a, axis, by):
    n = lax.axis_size(axis)
    return lax.ppermute(a, axis, [(i, (i + by) % n) for i in range(n)])


def spread(a, axis):
    return lax.all_to_all(a, axis, 0, 0, tiled=True)


def steps_of(tq, lq, hq, tk, lk, hk, tv, lv, hv, nt, ns):
    nz, nx = lax.axis_size("z"), lax.axis_size("x")
    rows, q_wide = tq.shape
    kv = tk.shape[1]
    wide = nx * rows
    a_wide = 2 * kv + A_Q * LANES
    bf = jnp.bfloat16
    low_q, low_k, low_v = lq.T, lk.T, lv.T
    part = nt.shape[0]
    b, a = call(
        merge_kernel,
        (tq, low_q, hq, tk, low_k, hk, tv, low_v, hv, nt[None], ns[None]),
        [VM, VM],
        [
            jax.ShapeDtypeStruct((nz, (q_wide // LANES - A_Q) * rows, LANES), bf),
            jax.ShapeDtypeStruct((rows + NORM_ROWS, a_wide), bf),
        ],
        vmem=None,
    )
    b1 = [spread(b, "z")]
    a = lax.all_gather(a, "x")
    own, own_norm = call(
        functools.partial(turn_kernel, rows, part),
        (a,),
        [VM, VM],
        [
            jax.ShapeDtypeStruct((a_wide + NORM_ROWS, wide), bf),
            jax.ShapeDtypeStruct((NORM_ROWS, nx * part), bf),
        ],
    )
    blocks = {0: own}
    for step in range(1, nz // 2):
        blocks[-step] = shift(blocks[1 - step], "z", 1)
        blocks[step] = shift(blocks[step - 1], "z", -1)
    blocks[-(nz // 2)] = shift(blocks[1 - nz // 2], "z", 1)
    b2 = []
    for b in b1:
        wide_b = call(
            fan_kernel,
            (b,),
            HBM,
            jax.ShapeDtypeStruct((nx, *b.shape), bf),
            scratch=[pltpu.SemaphoreType.DMA((nx,))],
        )
        b2.append(spread(wide_b, "x"))
    q_shape = jax.ShapeDtypeStruct((q_wide, nz * wide), bf)
    kv_shape = jax.ShapeDtypeStruct((kv, nz * wide), bf)

    def place_b(k, out_q):
        first = A_Q + sum(B_CUTS[:k])
        cut = B_CUTS[k]
        ins = (b2[k],) if out_q is None else (b2[k], out_q)
        return call(
            functools.partial(place_b_kernel, first, cut, rows),
            ins,
            ANY,
            q_shape,
            scratch=[pltpu.VMEM((cut * LANES, nz * wide), bf), pltpu.SemaphoreType.DMA((cut,))],
            aliases={} if out_q is None else {1: 0},
            n_any=len(ins) - 1,
        )

    half = nz // 2
    early = tuple(range(1 - half, half))
    far = shift(own_norm, "z", half)
    out_q, out_k, out_v, norm = call(
        functools.partial(early_kernel, early, nz, wide, kv),
        tuple(blocks[s] for s in early) + (far,),
        [ANY] * 3 + [VM],
        [q_shape, kv_shape, kv_shape, jax.ShapeDtypeStruct((nz, nx * part), bf)],
        scratch=[
            pltpu.VMEM((nz, nx * part), jnp.float32),
            pltpu.SemaphoreType.DMA((len(early), 3)),
        ],
    )
    other = lax.ppermute(norm, "tp", [(0, 1), (1, 0)])
    serve_norm = call(
        functools.partial(norm_kernel, part),
        (norm, other),
        VM,
        jax.ShapeDtypeStruct((nz, wide), bf),
    ).reshape(-1)
    for k in range(len(B_CUTS)):
        out_q = place_b(k, out_q)
    serve_query, serve_key, serve_value = call(
        functools.partial(late_kernel, (-half,), nz, wide, kv),
        (blocks[-half], out_q, out_k, out_v),
        [ANY] * 3,
        [q_shape, kv_shape, kv_shape],
        scratch=[pltpu.SemaphoreType.DMA((1, 3))],
        aliases={1 + i: i for i in range(3)},
        n_any=3,
    )
    return serve_query, serve_key, serve_value, serve_norm


def solution(mesh):
    rows, tp, job = mesh.devices.shape
    nx = 4
    fine = Mesh(mesh.devices.reshape(rows // nx, nx, tp, job), ("z", "x", "tp", "job"))
    r = ("job", "z", "x")
    w, low, high, vec = P(r, "tp"), P(r, None), P("job", "tp"), P(("job", "z", "x", "tp"))
    out_specs = (P(("job", "tp"), None),) * 3 + (P("job"),)
    return jax.shard_map(
        steps_of,
        mesh=fine,
        in_specs=(w, low, high) * 3 + (vec, vec),
        out_specs=out_specs,
        check_vma=False,
    )
```

```python
import functools

import jax
import jax.numpy as jnp
from jax import lax
from jax.experimental import pallas as pl
from jax.experimental.pallas import tpu as pltpu
from jax.sharding import Mesh, PartitionSpec as P


mix_rate = 0.5
LANES = 128
NORM_ROWS = 8
A_Q = 2


def merged(t, l, h, lo, hi):
    low_high = lax.dot_general(
        l[...], h[:, lo:hi], (((0,), (0,)), ((), ())), preferred_element_type=jnp.float32
    )
    return (t[:, lo:hi].astype(jnp.float32) + mix_rate * low_high).astype(jnp.bfloat16)


def merge_kernel(tq, lq, hq, tk, lk, hk, tv, lv, hv, nt, ns, out_b, out_a):
    rows = tq.shape[0]
    w = merged(tq, lq, hq, A_Q * LANES, tq.shape[1])
    for d in range(out_b.shape[0]):
        for j in range(w.shape[1] // LANES):
            out_b[d, j * rows : (j + 1) * rows, :] = w[:, j * LANES : (j + 1) * LANES]
    at = 0
    for t, l, h, width in (
        (tk, lk, hk, tk.shape[1]),
        (tv, lv, hv, tv.shape[1]),
        (tq, lq, hq, A_Q * LANES),
    ):
        out_a[:rows, at : at + width] = merged(t, l, h, 0, width)
        at += width
    norm = nt[...] + ns[...]
    norm = jnp.concatenate([norm, jnp.zeros((1, LANES - norm.shape[1]), jnp.float32)], axis=1)
    norm = jnp.broadcast_to(norm, (NORM_ROWS, LANES)).astype(jnp.bfloat16)
    out_a[rows:, :LANES] = norm
    out_a[rows:, LANES:] = jnp.zeros((NORM_ROWS, out_a.shape[1] - LANES), jnp.bfloat16)


def turn_kernel(rows, part, a, out, out_norm):
    n, _, width = a.shape
    for j in range(width // LANES):
        block = jnp.concatenate(
            [a[x, :rows, j * LANES : (j + 1) * LANES] for x in range(n)], axis=0
        )
        out[j * LANES : (j + 1) * LANES, :] = block.T
    norm = jnp.concatenate([a[x, rows:, :part] for x in range(n)], axis=1)
    out_norm[...] = norm
    out[width:, : n * part] = norm
    out[width:, n * part :] = jnp.zeros((NORM_ROWS, out.shape[1] - n * part), jnp.bfloat16)


def place_b_kernel(first, cut, rows, nx, own, below, above, far_low, far_high, *rest):
    out, held, sem = rest[-3:]
    nz = own.shape[0]
    wide = nx * rows
    half = nz // 2

    def piece(step, z, at):
        if step == nx // 2:
            return far_low[z, at, :] if z < half else far_high[z - half, at, :]
        return {0: own, 1: above, nx - 1: below}[step][z, at, :]

    def turn_all(me):
        for j in range(cut):
            at = slice(j * rows, (j + 1) * rows)
            for z in range(nz):
                block = jnp.concatenate([piece((x - me) % nx, z, at) for x in range(nx)], axis=0)
                held[j * LANES : (j + 1) * LANES, z * wide : (z + 1) * wide] = block.T
            row_copy(j).start()

    def row_copy(j):
        return pltpu.make_async_copy(
            held.at[pl.ds(j * LANES, LANES), :],
            out.at[pl.ds((first + j) * LANES, LANES), :],
            sem.at[j],
        )

    for me in range(nx):
        pl.when(lax.axis_index("x") == me)(functools.partial(turn_all, me))
    for j in range(cut):
        row_copy(j).wait()


def place_a(steps, nz, wide, kv, blocks, out_q, out_k, out_v, sem):
    me = lax.axis_index("z")
    end = 2 * kv + A_Q * LANES
    copies = []
    for i, (step, block) in enumerate(zip(steps, blocks)):
        z = lax.rem(me + (step + nz), nz)
        at = pl.ds(pl.multiple_of(z * wide, wide), wide)
        for s, (lo, hi, out) in enumerate(
            ((0, kv, out_k), (kv, 2 * kv, out_v), (2 * kv, end, out_q))
        ):
            copy = pltpu.make_async_copy(
                block.at[pl.ds(lo, hi - lo), :], out.at[pl.ds(0, hi - lo), at], sem.at[i, s]
            )
            copy.start()
            copies.append(copy)
    return copies


def early_kernel(steps, nz, wide, kv, *refs):
    n = len(steps)
    blocks, far = refs[:n], refs[n]
    out_q, out_k, out_v, out_n, held, sem = refs[n + 1 :]
    copies = place_a(steps, nz, wide, kv, blocks, out_q, out_k, out_v, sem)
    me = lax.axis_index("z")
    end = 2 * kv + A_Q * LANES
    lanes = held.shape[1]
    rows = [block[end:, :lanes] for block in blocks] + [far[...]]
    for step, row in zip(steps + (nz // 2,), rows):
        held[pl.ds(lax.rem(me + (step + nz), nz), 1), :] = row.astype(jnp.float32)[:1, :]
    out_n[...] = held[...].astype(out_n.dtype)
    for copy in copies:
        copy.wait()


def late_kernel(steps, nz, wide, kv, *refs):
    n = len(steps)
    copies = place_a(steps, nz, wide, kv, refs[:n], *refs[-4:])
    for copy in copies:
        copy.wait()


def norm_kernel(part, mine, other, out):
    m, o = mine[...].astype(jnp.float32), other[...].astype(jnp.float32)
    first = lax.axis_index("tp") == 0
    halves = (jnp.where(first, m, o), jnp.where(first, o, m))
    pieces = []
    for x in range(m.shape[1] // part):
        pieces += [half[:, x * part : (x + 1) * part] for half in halves]
    out[...] = jnp.concatenate(pieces, axis=1).astype(out.dtype)


VM = pl.BlockSpec(memory_space=pltpu.VMEM)
ANY = pl.BlockSpec(memory_space=pl.ANY)


def call(kernel, ins, out_specs, out_shape, scratch=(), aliases={}, n_any=0, cost=1 << 20, vmem=16 << 20):
    return pl.pallas_call(
        kernel,
        in_specs=[VM] * (len(ins) - n_any) + [ANY] * n_any,
        out_specs=out_specs,
        out_shape=out_shape,
        scratch_shapes=list(scratch),
        input_output_aliases=aliases,
        compiler_params=pltpu.CompilerParams(vmem_limit_bytes=vmem),
        cost_estimate=pl.CostEstimate(flops=cost, bytes_accessed=cost, transcendentals=0),
    )(*ins)


def shift(a, axis, by):
    n = lax.axis_size(axis)
    return lax.ppermute(a, axis, [(i, (i + by) % n) for i in range(n)])


def spread(a, axis):
    return lax.all_to_all(a, axis, 0, 0, tiled=True)


def steps_of(tq, lq, hq, tk, lk, hk, tv, lv, hv, nt, ns):
    nz, nx = lax.axis_size("z"), lax.axis_size("x")
    rows, q_wide = tq.shape
    kv = tk.shape[1]
    wide = nx * rows
    a_wide = 2 * kv + A_Q * LANES
    bf = jnp.bfloat16
    low_q, low_k, low_v = lq.T, lk.T, lv.T
    part = nt.shape[0]
    b, a = call(
        merge_kernel,
        (tq, low_q, hq, tk, low_k, hk, tv, low_v, hv, nt[None], ns[None]),
        [VM, VM],
        [
            jax.ShapeDtypeStruct((nz, (q_wide // LANES - A_Q) * rows, LANES), bf),
            jax.ShapeDtypeStruct((rows + NORM_ROWS, a_wide), bf),
        ],
        vmem=None,
    )
    b = spread(b, "z")
    a = lax.all_gather(a, "x")
    own, own_norm = call(
        functools.partial(turn_kernel, rows, part),
        (a,),
        [VM, VM],
        [
            jax.ShapeDtypeStruct((a_wide + NORM_ROWS, wide), bf),
            jax.ShapeDtypeStruct((NORM_ROWS, nx * part), bf),
        ],
    )
    blocks = {0: own}
    for step in range(1, nz // 2):
        blocks[-step] = shift(blocks[1 - step], "z", 1)
        blocks[step] = shift(blocks[step - 1], "z", -1)
    blocks[-(nz // 2)] = shift(blocks[1 - nz // 2], "z", 1)
    b_p = shift(b, "x", 1)
    b_m = shift(b, "x", -1)
    b_rp = shift(b_p[: nz // 2], "x", 1)
    b_rm = shift(b_m[nz // 2 :], "x", -1)
    q_shape = jax.ShapeDtypeStruct((q_wide, nz * wide), bf)
    kv_shape = jax.ShapeDtypeStruct((kv, nz * wide), bf)

    half = nz // 2
    early = tuple(range(1 - half, half))
    far = shift(own_norm, "z", half)
    out_q, out_k, out_v, norm = call(
        functools.partial(early_kernel, early, nz, wide, kv),
        tuple(blocks[s] for s in early) + (far,),
        [ANY] * 3 + [VM],
        [q_shape, kv_shape, kv_shape, jax.ShapeDtypeStruct((nz, nx * part), bf)],
        scratch=[
            pltpu.VMEM((nz, nx * part), jnp.float32),
            pltpu.SemaphoreType.DMA((len(early), 3)),
        ],
    )
    other = lax.ppermute(norm, "tp", [(0, 1), (1, 0)])
    serve_norm = call(
        functools.partial(norm_kernel, part),
        (norm, other),
        VM,
        jax.ShapeDtypeStruct((nz, wide), bf),
    ).reshape(-1)
    cut = q_wide // LANES - A_Q
    out_q = call(
        functools.partial(place_b_kernel, A_Q, cut, rows, nx),
        (b, b_p, b_m, b_rp, b_rm, out_q),
        ANY,
        q_shape,
        scratch=[
            pltpu.VMEM((cut * LANES, nz * wide), bf),
            pltpu.SemaphoreType.DMA((cut,)),
        ],
        aliases={5: 0},
        n_any=1,
    )
    serve_query, serve_key, serve_value = call(
        functools.partial(late_kernel, (-half,), nz, wide, kv),
        (blocks[-half], out_q, out_k, out_v),
        [ANY] * 3,
        [q_shape, kv_shape, kv_shape],
        scratch=[pltpu.SemaphoreType.DMA((1, 3))],
        aliases={1 + i: i for i in range(3)},
        n_any=3,
    )
    return serve_query, serve_key, serve_value, serve_norm


def solution(mesh):
    rows, tp, job = mesh.devices.shape
    nx = 4
    fine = Mesh(mesh.devices.reshape(rows // nx, nx, tp, job), ("z", "x", "tp", "job"))
    r = ("job", "z", "x")
    w, low, high, vec = P(r, "tp"), P(r, None), P("job", "tp"), P(("job", "z", "x", "tp"))
    out_specs = (P(("job", "tp"), None),) * 3 + (P("job"),)
    return jax.shard_map(
        steps_of,
        mesh=fine,
        in_specs=(w, low, high) * 3 + (vec, vec),
        out_specs=out_specs,
        check_vma=False,
    )
```
